128 devices in a mesh: groups: 4 (over y, x), gx: 16 (over z), gy: 2 (over core).
Axes of the slice: x: 2, y: 2, z: 16, core: 2. Of those that a mesh axis runs over, the one named last changes fastest.
The devices are a block of a 8x8x16 slice.
Arguments:
- source: float32 [4, 3, 2, 64, 64, 256], P('groups', None, None, 'gx', 'gy'), parts along dimension 0, may hold values from -12 to 12
- permittivity: float32 [12, 64, 64, 256], P('groups', 'gx', 'gy'), parts along dimension 0, may hold values from 1 to 12
- frequency: float32 [1], replicated, may hold values from 0.25 to 0.6
Outputs:
- solution: float32 [4, 3, 2, 64, 64, 256], P('groups', None, None, 'gx', 'gy'), parts along dimension 0
- residual: float32 [4, 3, 2, 64, 64, 256], P('groups', None, None, 'gx', 'gy'), parts along dimension 0
The draws below stay inside these ranges and needn't reach their ends.
There are 4 independent parts, one for each index of `groups`. The reference program is written for one: setup_inputs(seed, part) draws one part's arguments, and reference() takes and returns one part's arrays. A program takes and returns all parts, laid end to end along the dimension named above; an argument that names none is the same for every part. Nothing has to cross between parts.
All inputs are finite; a program needn't handle non-finite values.
Results may differ from the reference program's by a relative error of at most 0.0003.
Values sent between devices are 32-bit elements; how exact they have to be, the bound alone decides.
No kernel may reach another device: no remote copies, remote signals or barrier semaphores. Data moves between devices by JAX's collectives and lax.ppermute only.
A program may use at most 64 MiB of HBM per device.

```python
import jax
import jax.numpy as jnp

WAVES = 1
NZ = 256
PML = 8
ITERS = 3
NX = 64
NY = 64


def draw_source(key, part):
    noise_key = jax.random.fold_in(jax.random.fold_in(key, 17), 0)
    target = (WAVES, 3, 2, NX, NY, NZ)
    place_x = jnp.arange(NX, dtype=jnp.int32).astype(jnp.float32) / max(NX - 1, 1)
    rising = (1.0 + 2.0 * place_x).reshape(1, 1, 1, NX, 1, 1)
    return (jax.random.truncated_normal(noise_key, -4.0, 4.0, target, jnp.float32) * rising).astype(jnp.float32)


def steps_of(rng, extent, shards, smallest, top_value):
    def one(axis_at, parts):
        steps = jax.random.uniform(jax.random.fold_in(jax.random.fold_in(rng, 6), axis_at), (parts,), jnp.float32, smallest / len(shards), top_value / len(shards))
        return jnp.repeat(jnp.exp(steps), extent[axis_at] // parts).reshape((-1,) + (1,) * (len(extent) - axis_at - 1))

    factor_of = one(*shards[0])
    for cut in shards[1:]:
        factor_of = factor_of * one(*cut)
    return factor_of


def setup_inputs(seed: int = 0, part: int = 0) -> dict:
    splits = jax.random.split(jax.random.key(seed), 4)
    part_keys = jax.random.split(jax.random.fold_in(splits[3], part), 4)
    source = draw_source(jax.random.fold_in(jax.random.fold_in(splits[3], part), 71), part)
    permittivity = jnp.clip(1.0 + 11.0 * jax.random.uniform(part_keys[1], (3, NX, NY, NZ), jnp.float32) ** steps_of(part_keys[1], (3, NX, NY, NZ), ((1, 16), (2, 2)), -0.2, 0.2), 1.0, 12.0)
    frequency = jnp.clip(jax.random.uniform(splits[2], (WAVES,), jnp.float32, 0.25, 0.6), 0.25, 0.6)
    return {"source": source, "permittivity": permittivity, "frequency": frequency}


pml_strength = 2.0


def stretch(points, length, frequency):
    inside = jnp.maximum(jnp.maximum(PML - points, points - (length - PML)), 0.0) / PML
    damping = pml_strength * inside ** 3 / frequency[:, None]
    factor = 1.0 / (1.0 + damping * damping)
    return jnp.stack([factor, -damping * factor], axis=1)


def orient(coefficient, dimension):
    target = [coefficient.shape[0], 2, 1, 1, 1]
    target[dimension] = coefficient.shape[2]
    return coefficient.reshape(target)


def times_coef(values, coefficient):
    real_part = values[:, 0] * coefficient[:, 0] - values[:, 1] * coefficient[:, 1]
    imag_part = values[:, 0] * coefficient[:, 1] + values[:, 1] * coefficient[:, 0]
    return jnp.stack([real_part, imag_part], axis=1)


def curl_forward(extended, front_x, front_y, front_z):
    centre = extended[:, :, :, :-1, :-1]

    def step_x(component):
        return extended[:, component, :, 1:, :-1] - centre[:, component]

    def step_y(component):
        return extended[:, component, :, :-1, 1:] - centre[:, component]

    def step_z(component):
        cells = centre[:, component]
        above = jnp.concatenate([cells[..., 1:], jnp.zeros_like(cells[..., :1])], axis=-1)
        return above - cells

    curl_x = times_coef(step_y(2), front_y) - times_coef(step_z(1), front_z)
    curl_y = times_coef(step_z(0), front_z) - times_coef(step_x(2), front_x)
    curl_z = times_coef(step_x(1), front_x) - times_coef(step_y(0), front_y)
    return jnp.stack([curl_x, curl_y, curl_z], axis=1)


def curl_backward(padded, back_x, back_y, back_z):
    centre = padded[:, :, :, 1:, 1:]

    def step_x(component):
        return centre[:, component] - padded[:, component, :, :-1, 1:]

    def step_y(component):
        return centre[:, component] - padded[:, component, :, 1:, :-1]

    def step_z(component):
        cells = centre[:, component]
        below = jnp.concatenate([jnp.zeros_like(cells[..., :1]), cells[..., :-1]], axis=-1)
        return cells - below

    out_x = times_coef(step_y(2), back_y) - times_coef(step_z(1), back_z)
    out_y = times_coef(step_z(0), back_z) - times_coef(step_x(2), back_x)
    out_z = times_coef(step_x(1), back_x) - times_coef(step_y(0), back_y)
    return jnp.stack([out_x, out_y, out_z], axis=1)


def scaled(values, number):
    real_scale = number[0].reshape(-1, 1, 1, 1, 1)
    imag_scale = number[1].reshape(-1, 1, 1, 1, 1)
    real_part = values[:, :, 0] * real_scale - values[:, :, 1] * imag_scale
    imag_part = values[:, :, 0] * imag_scale + values[:, :, 1] * real_scale
    return jnp.stack([real_part, imag_part], axis=2)


def product(left, right):
    real_part = jnp.sum(left[:, :, 0] * right[:, :, 0] + left[:, :, 1] * right[:, :, 1], axis=(1, 2, 3, 4))
    imag_part = jnp.sum(left[:, :, 0] * right[:, :, 1] - left[:, :, 1] * right[:, :, 0], axis=(1, 2, 3, 4))
    return jnp.stack([real_part, imag_part])


def complex_times(first, other):
    return jnp.stack([first[0] * other[0] - first[1] * other[1], first[0] * other[1] + first[1] * other[0]])


def complex_ratio(first, other):
    modulus = other[0] * other[0] + other[1] * other[1]
    return jnp.stack([first[0] * other[0] + first[1] * other[1], first[1] * other[0] - first[0] * other[1]]) / modulus


def grid_factors(length, frequency, dimension):
    points = jnp.arange(length, dtype=jnp.int32).astype(jnp.float32)
    front = orient(stretch(points + 0.5, length, frequency), dimension)
    back = orient(stretch(points, length, frequency), dimension)
    return front, back


def reference(source, permittivity, frequency):
    front_x, back_x = grid_factors(NX, frequency, 2)
    front_y, back_y = grid_factors(NY, frequency, 3)
    front_z, back_z = grid_factors(NZ, frequency, 4)

    def operate(values):
        extended = jnp.pad(values, ((0, 0), (0, 0), (0, 0), (0, 1), (0, 1), (0, 0)))
        rotated = curl_forward(extended, front_x, front_y, front_z)
        padded = jnp.pad(rotated, ((0, 0), (0, 0), (0, 0), (1, 0), (1, 0), (0, 0)))
        applied = curl_backward(padded, back_x, back_y, back_z)
        return applied - (frequency * frequency).reshape(-1, 1, 1, 1, 1, 1) * permittivity[None, :, None] * values

    solution = jnp.zeros_like(source)
    residual = source
    shadow = source
    direction = source
    shadow_dot = product(shadow, residual)
    for iteration in range(ITERS):
        applied = operate(direction)
        step_size = complex_ratio(shadow_dot, product(shadow, applied))
        middle = residual - scaled(applied, step_size)
        second = operate(middle)
        weight = complex_ratio(product(second, middle), product(second, second))
        solution = solution + scaled(direction, step_size) + scaled(middle, weight)
        residual = middle - scaled(second, weight)
        if iteration + 1 < ITERS:
            shadow_next = product(shadow, residual)
            momentum = complex_times(complex_ratio(shadow_next, shadow_dot), complex_ratio(step_size, weight))
            direction = residual + scaled(direction - scaled(applied, weight), momentum)
            shadow_dot = shadow_next
    return solution, residual
```

```python
import functools

import jax
import jax.numpy as jnp
from jax import lax
from jax.experimental import pallas as pl
from jax.experimental.pallas import tpu as pltpu
from jax.sharding import PartitionSpec as P

PML = 8
ITERS = 3
DEGREE = 2 * ITERS
pml_strength = 2.0
LANES = 128
TILE = 8

NODES = (0.0, -1.0, 1.0, 0.577, -0.671, 0.319)
F32 = jnp.float32
VMEM = pl.BlockSpec(memory_space=pltpu.VMEM)
ANY = pl.BlockSpec(memory_space=pl.ANY)


def params(mib):
    return pltpu.CompilerParams(vmem_limit_bytes=mib * 2**20)


def stretch(points, length, frequency):
    inside = jnp.maximum(jnp.maximum(PML - points, points - (length - PML)), 0.0) / PML
    damping = pml_strength * inside * inside * inside / frequency
    factor = 1.0 / (1.0 + damping * damping)
    return factor, -damping * factor


def times(value, factor):
    return (
        value[0] * factor[0] - value[1] * factor[1],
        value[0] * factor[1] + value[1] * factor[0],
    )


def minus(a, b):
    return a[0] - b[0], a[1] - b[1]


def plus(a, b):
    return a[0] + b[0], a[1] + b[1]


def iota(shape, axis):
    return lax.broadcasted_iota(jnp.int32, shape, axis)


class Line:
    def __init__(self):
        self.lane = iota((TILE, LANES), 1)
        self.row = iota((TILE, LANES), 0)
        self.zero = jnp.zeros((TILE, LANES), F32)

    def z_next(self, low, high):
        low, high = pltpu.roll(low, LANES - 1, 1), pltpu.roll(high, LANES - 1, 1)
        last = self.lane == LANES - 1
        return jnp.where(last, high, low), jnp.where(last, 0.0, high)

    def z_before(self, low, high):
        low, high = pltpu.roll(low, 1, 1), pltpu.roll(high, 1, 1)
        first = self.lane == 0
        return jnp.where(first, 0.0, low), jnp.where(first, low, high)

    def up(self, tile):
        return pltpu.roll(tile, TILE - 1, 0)

    def down(self, tile):
        return pltpu.roll(tile, 1, 0)

    def y_next(self, rolled, rolled_after):
        return jnp.where(self.row == TILE - 1, rolled_after, rolled)

    def y_before(self, rolled, rolled_ahead):
        return jnp.where(self.row == 0, rolled_ahead, rolled)


def z_steps(line, pair):
    out = []
    for part in range(2):
        low, high = pair[0][part], pair[1][part]
        a, b = line.z_next(low, high)
        out.append((a - low, b - high))
    return [(out[0][h], out[1][h]) for h in range(2)]


def z_steps_back(line, pair):
    out = []
    for part in range(2):
        low, high = pair[0][part], pair[1][part]
        a, b = line.z_before(low, high)
        out.append((low - a, high - b))
    return [(out[0][h], out[1][h]) for h in range(2)]


def row_of(ref, at):
    return jnp.broadcast_to(ref[at : at + 1, :], (TILE, LANES))


def complex_row(ref, at):
    return row_of(ref, at), row_of(ref, at + 1)


def is_stretched(t, tiles):
    return t * TILE < PML or (t + 1) * TILE > tiles * TILE - PML


def edge_terms(line, field, t, tiles, fz, fx, y_front, store):
    now = field(t)
    after = field(t + 1) if t + 1 < tiles else None
    dz = z_steps(line, now[0])
    for h in range(2):
        gy = plus(times(dz[h], fz[h]), times(now[2][h], fx))
        dy = []
        for part in range(2):
            rolled = line.up(now[0][h][part])
            nxt = line.up(after[0][h][part]) if after is not None else line.zero
            dy.append(line.y_next(rolled, nxt) - now[0][h][part])
        if is_stretched(t, tiles):
            dy = times(dy, y_front(t))
        gz = minus((-dy[0], -dy[1]), times(now[1][h], fx))
        for part in range(2):
            store(0, part, h, t, gy[part])
            store(1, part, h, t, gz[part])


def tile_reader(ref, components=3):
    def read(t):
        s = slice(t * TILE, (t + 1) * TILE)
        return [
            [(ref[c, 0, h, s, :], ref[c, 1, h, s, :]) for h in range(2)] for c in range(components)
        ]

    return read


def tile_writer(ref):
    def write(c, part, h, t, value):
        ref[c, part, h, t * TILE : (t + 1) * TILE, :] = value

    return write


def start_kernel(
    cells_x, src, eps, src_in, eps_in, freq,
    o_ref, n_ref, mo_ref, mn_ref, go_ref, gn_ref, off_ref, on_ref, cy_ref, cz_ref, cx_ref, ct_ref,
):
    core = lax.axis_index("gy")
    chip = lax.axis_index("gx")
    rows, cols = src.shape[4], src.shape[5]
    ny, nx = 2 * rows, cells_x * lax.axis_size("gx")
    half_x = cells_x // 2
    tiles = ny // TILE
    f = jnp.broadcast_to(freq[...], (TILE, LANES))
    square = f * f

    def arrange(first_own):
        own_rows = slice(rows * first_own, rows * (first_own + 1))
        other_rows = slice(rows * (1 - first_own), rows * (2 - first_own))
        for dest, mdest, plane in ((o_ref, mo_ref, first_own), (n_ref, mn_ref, 1 - first_own)):
            for h in range(2):
                z = slice(h * LANES, (h + 1) * LANES)
                for c in range(3):
                    for part in range(2):
                        dest[c, part, h, own_rows, :] = src[0, c, part, half_x * first_own + plane, :, z]
                        dest[c, part, h, other_rows, :] = src_in[c, part, plane, :, z]
                    scale = square[0:1, :]
                    mdest[c, h, own_rows, :] = eps[c, half_x * first_own + plane, :, z] * scale
                    mdest[c, h, other_rows, :] = eps_in[c, plane, :, z] * scale

    @pl.when(core == 0)
    def _():
        arrange(0)

    @pl.when(core != 0)
    def _():
        arrange(1)

    fy = jnp.broadcast_to(freq[...], (ny, LANES))
    y = iota((ny, LANES), 0).astype(F32)
    cy_ref[0], cy_ref[1] = stretch(y + 0.5, ny, fy)
    cy_ref[2], cy_ref[3] = stretch(y, ny, fy)
    lane = iota((TILE, LANES), 1)
    for h in range(2):
        z = (lane + h * LANES).astype(F32)
        for i, value in enumerate((*stretch(z + 0.5, cols, f), *stretch(z, cols, f))):
            cz_ref[4 * h + i : 4 * h + i + 1, :] = value[0:1, :]
    base = chip * cells_x + core * half_x
    for at, plane in ((0, core), (TILE, 1 - core)):
        x = (jnp.zeros((TILE, LANES), jnp.int32) + (base + plane)).astype(F32)
        values = (*stretch(x - 0.5, nx, f), *stretch(x + 0.5, nx, f), *stretch(x, nx, f))
        for i, value in enumerate(values):
            cx_ref[at + i : at + i + 1, :] = value[0:1, :]
    low = square * -12.0
    centre, radius = (12.0 + low) * 0.5, (12.0 - low) * 0.5
    for k, node in enumerate(NODES):
        ct_ref[k : k + 1, :] = (centre + radius * node)[0:1, :]
    ct_ref[DEGREE : DEGREE + 1, :] = (2.0 / radius)[0:1, :]

    line = Line()
    fz = [complex_row(cz_ref, 4 * h) for h in range(2)]

    def y_front(t):
        s = slice(t * TILE, (t + 1) * TILE)
        return cy_ref[0, s, :], cy_ref[1, s, :]

    for ref, g_ref, at in ((o_ref, go_ref, 0), (n_ref, gn_ref, TILE)):
        for t in range(tiles):
            edge_terms(
                line, tile_reader(ref), t, tiles, fz, complex_row(cx_ref, at + 2), y_front,
                tile_writer(g_ref),
            )

    @pl.when(core == 0)
    def _():
        off_ref[...] = o_ref[1:3]
        on_ref[...] = gn_ref[...]

    @pl.when(core != 0)
    def _():
        off_ref[...] = go_ref[...]
        on_ref[...] = n_ref[1:3]


def plane_kernel(
    outer, k, p_ref, q_ref, gq_ref, halo_ref, m_ref, cy_ref, cz_ref, cx_ref, ct_ref,
    new_ref, g_ref, out_ref,
):
    core = lax.axis_index("gy")
    chip = lax.axis_index("gx")
    tiles = p_ref.shape[3] // TILE
    at = 0 if outer else TILE
    line = Line()
    before = complex_row(cx_ref, at)
    fx = complex_row(cx_ref, at + 2)
    bx = complex_row(cx_ref, at + 4)
    fz = [complex_row(cz_ref, 4 * h) for h in range(2)]
    bz = [complex_row(cz_ref, 4 * h + 2) for h in range(2)]
    node = row_of(ct_ref, k)
    scale = row_of(ct_ref, DEGREE)

    def y_factor(first, t):
        s = slice(t * TILE, (t + 1) * TILE)
        return cy_ref[first, s, :], cy_ref[first + 1, s, :]

    def run(left):
        zero = line.zero
        edge = left and outer
        wall = outer and not left
        at_edge = (chip == 0) if edge else (chip == lax.axis_size("gx") - 1)
        closed = jnp.zeros((TILE, LANES), jnp.int32) + at_edge.astype(jnp.int32) > 0
        read_p = tile_reader(p_ref)
        read_g = tile_reader(halo_ref if left else gq_ref, 2)
        if left:
            read_r = lambda t: tile_reader(q_ref)(t)[1:]
        else:
            read_r = tile_reader(halo_ref, 2)
        rolled_h = None
        pending = None
        nxt = read_p(0)
        rolled = [[[line.up(nxt[c][h][i]) for i in range(2)] for h in range(2)] for c in (0, 2)]
        write_new, write_g, write_out = tile_writer(new_ref), tile_writer(g_ref), tile_writer(out_ref)
        write_edge = write_g if left else write_out

        def finish(pend, after):
            t0, ex, rolled_ex, base = pend
            for h in range(2):
                dy = [
                    line.y_next(rolled_ex[h][i], after[h][i] if after is not None else zero) - ex[h][i]
                    for i in range(2)
                ]
                if is_stretched(t0, tiles):
                    dy = times(dy, y_factor(0, t0))
                for i in range(2):
                    write_edge(1, i, h, t0, base[h][i] - dy[i])

        for t in range(tiles):
            ex, ey, ez = nxt
            if t + 1 < tiles:
                nxt = read_p(t + 1)
                rolled_next = [
                    [[line.up(nxt[c][h][i]) for i in range(2)] for h in range(2)] for c in (0, 2)
                ]
            else:
                rolled_next = [[[zero] * 2] * 2] * 2
            gl, right = read_g(t), read_r(t)
            pml = is_stretched(t, tiles)
            dz_y, dz_x = z_steps(line, ey), z_steps(line, ex)
            hx, hy, hz, cross_y, cross_z = [], [], [], [], []
            for h in range(2):
                dy_x, dy_z = (
                    [
                        line.y_next(rolled[j][h][i], rolled_next[j][h][i]) - field[h][i]
                        for i in range(2)
                    ]
                    for j, field in ((0, ex), (1, ez))
                )
                if pml:
                    dy_x, dy_z = times(dy_x, y_factor(0, t)), times(dy_z, y_factor(0, t))
                r_y, r_z = right[0][h], right[1][h]
                if wall:
                    r_y = [jnp.where(closed, 0.0, r) for r in r_y]
                    r_z = [jnp.where(closed, 0.0, r) for r in r_z]
                hx.append(minus(dy_z, times(dz_y[h], fz[h])))
                hy.append(minus(times(dz_x[h], fz[h]), times(minus(r_z, ez[h]), fx)))
                hz.append(minus(times(minus(r_y, ey[h]), fx), dy_x))
                l_y = minus(gl[0][h], times(ez[h], before))
                l_z = plus(gl[1][h], times(ey[h], before))
                if edge:
                    l_y = [jnp.where(closed, 0.0, v) for v in l_y]
                    l_z = [jnp.where(closed, 0.0, v) for v in l_z]
                cross_y.append(times(minus(hy[h], l_y), bx))
                cross_z.append(times(minus(hz[h], l_z), bx))
            rolled = rolled_next
            new_rolled = [[[line.down(v[h][i]) for i in range(2)] for h in range(2)] for v in (hx, hz)]
            bz_y, bz_x = z_steps_back(line, hy), z_steps_back(line, hx)
            s = slice(t * TILE, (t + 1) * TILE)
            made = [[], [], []]
            for h in range(2):
                by_x, by_z = (
                    [
                        field[h][i]
                        - line.y_before(
                            new_rolled[j][h][i], rolled_h[j][h][i] if rolled_h is not None else zero
                        )
                        for i in range(2)
                    ]
                    for j, field in ((0, hx), (1, hz))
                )
                if pml:
                    by_x, by_z = times(by_x, y_factor(2, t)), times(by_z, y_factor(2, t))
                curls = (
                    minus(by_z, times(bz_y[h], bz[h])),
                    minus(times(bz_x[h], bz[h]), cross_z[h]),
                    minus(cross_y[h], by_x),
                )
                for c, (curl, field) in enumerate(zip(curls, (ex, ey, ez))):
                    shifted = m_ref[c, h, s, :] + node
                    made[c].append([(curl[i] - shifted * field[h][i]) * scale for i in range(2)])
                    for i in range(2):
                        write_new(c, i, h, t, made[c][h][i])
                        if left and c:
                            write_out(c - 1, i, h, t, made[c][h][i])
            rolled_h = new_rolled
            dz = z_steps(line, made[0])
            up = [[line.up(made[0][h][i]) for i in range(2)] for h in range(2)]
            base = []
            for h in range(2):
                gy = plus(times(dz[h], fz[h]), times(made[2][h], fx))
                for i in range(2):
                    write_edge(0, i, h, t, gy[i])
                b = times(made[1][h], fx)
                base.append((-b[0], -b[1]))
            if pending is not None:
                finish(pending, up)
            pending = (t, made[0], up, base)
        finish(pending, None)

    left_here = (core == 0) if outer else (core != 0)

    @pl.when(left_here)
    def _():
        run(True)

    @pl.when(jnp.logical_not(left_here))
    def _():
        run(False)


def two_sum(a, b):
    s = a + b
    v = s - a
    return s, (a - (s - v)) + (b - v)


def total_of(tile):
    top = jnp.max(jnp.max(jnp.abs(tile), axis=1, keepdims=True), axis=0, keepdims=True)
    shift = top * 1024.0
    lead = (tile + shift) - shift
    rest = tile - lead
    add = lambda v: jnp.sum(jnp.sum(v, axis=1, keepdims=True), axis=0, keepdims=True)
    return add(lead), add(rest)


def gram_kernel(k, copies, *refs):
    count = k + 1
    os, ns = refs[:count], refs[count : 2 * count]
    rest = list(refs[2 * count :])
    row_in = rest.pop(0) if k else None
    row_ref = rest.pop(0)
    core = lax.axis_index("gy")
    tiles = os[0].shape[3] // TILE
    zero = jnp.zeros((TILE, LANES), F32)
    real = [[zero, zero] for _ in range(count)]
    imag = [[zero, zero] for _ in range(count)]
    for which, group in enumerate((os, ns)):
        for c in range(3):
            for h in range(2):
                for t in range(tiles):
                    s = slice(t * TILE, (t + 1) * TILE)
                    ar, ai = group[k][c, 0, h, s, :], group[k][c, 1, h, s, :]
                    for i in range(k):
                        br, bi = group[i][c, 0, h, s, :], group[i][c, 1, h, s, :]
                        real[i][which] += br * ar + bi * ai
                        imag[i][which] += br * ai - bi * ar
                    real[k][which] += ar * ar + ai * ai
    lane = iota((1, LANES), 1)
    row = row_in[...] if k else jnp.zeros((1, LANES), F32)
    for i in range(count):
        lead, less = total_of(real[i][0] + real[i][1])
        row = jnp.where(lane == 8 * i + k, lead, row)
        row = jnp.where(lane == 64 + 8 * i + k, less, row)
        if i < k:
            lead, less = total_of(imag[i][0] + imag[i][1])
            row = jnp.where(lane == 8 * k + i, lead, row)
            row = jnp.where(lane == 64 + 8 * k + i, less, row)
    if copies == 1:
        row_ref[...] = row
    else:
        for d in range(copies):
            row_ref[d] = row
    if k:
        other_ref = rest.pop(0)
        half = other_ref.shape[4]
        first = pl.multiple_of(half * (1 - core), TILE)
        for which, group in enumerate((os, ns)):
            for c in range(3):
                for part in range(2):
                    for h in range(2):
                        other_ref[which, c, part, h] = group[k][c, part, h, pl.ds(first, half), :]


def quick(a, b):
    s = a + b
    return s, b - (s - a)


def add2(a, b):
    s, e = two_sum(a[0], b[0])
    return quick(s, e + (a[1] + b[1]))


def neg2(a):
    return -a[0], -a[1]


def split(a):
    c = a * 4097.0
    high = c - (c - a)
    return high, a - high


def mul2(a, b):
    p = a[0] * b[0]
    (a1, a2), (b1, b2) = split(a[0]), split(b[0])
    e = ((a1 * b1 - p) + a1 * b2 + a2 * b1) + a2 * b2
    return quick(p, e + (a[0] * b[1] + a[1] * b[0]))


def div2(a, b):
    q = a[0] / b[0]
    rest = add2(a, neg2(mul2((q, jnp.zeros_like(q)), b)))
    q2 = rest[0] / b[0]
    rest = add2(rest, neg2(mul2((q2, jnp.zeros_like(q)), b)))
    return add2(quick(q, q2), (rest[0] / b[0], jnp.zeros_like(q)))


def cadd(a, b):
    return add2(a[0], b[0]), add2(a[1], b[1])


def cneg(a):
    return neg2(a[0]), neg2(a[1])


def conj(a):
    return a[0], neg2(a[1])


def cmul(a, b):
    return (
        add2(mul2(a[0], b[0]), neg2(mul2(a[1], b[1]))),
        add2(mul2(a[0], b[1]), mul2(a[1], b[0])),
    )


def cdiv(a, b):
    size = add2(mul2(b[0], b[0]), mul2(b[1], b[1]))
    top = cmul(a, conj(b))
    return div2(top[0], size), div2(top[1], size)


def each(fn, a):
    return tuple((fn(p[0]), fn(p[1])) for p in a)


def over_rows(a):
    for d in (4, 2, 1):
        a = cadd(a, each(lambda v: pltpu.roll(v, d, 0), a))
    return a


def coefficients(gathered, ct_ref):
    parts = [gathered[i * TILE : (i + 1) * TILE] for i in range(gathered.shape[0] // TILE)]
    parts = [(p, jnp.zeros_like(p)) for p in parts]
    while len(parts) > 1:
        parts = [add2(parts[2 * i], parts[2 * i + 1]) for i in range(len(parts) // 2)]
    total = parts[0]
    for d in (4, 2, 1):
        total = add2(total, tuple(pltpu.roll(v, d, 0) for v in total))
    other = tuple(pltpu.roll(v, 64, 1) for v in total)
    total = add2(total, other)
    row, lane = iota((TILE, LANES), 0), iota((TILE, LANES), 1)

    def picked(mask):
        return tuple(
            jnp.broadcast_to(
                jnp.sum(jnp.where(mask, v, 0.0), axis=1, keepdims=True), (TILE, LANES)
            )
            for v in total
        )

    columns = []
    for j in range(DEGREE + 1):
        real = picked(lane == 8 * jnp.minimum(row, j) + jnp.maximum(row, j))
        imag = picked((lane == 8 * jnp.maximum(row, j) + jnp.minimum(row, j)) & (row != j))
        imag = tuple(jnp.where(row > j, -v, v) for v in imag)
        columns.append((real, imag))
    zero = jnp.zeros((TILE, LANES), F32)
    first_row = conj(columns[0])
    scale = row_of(ct_ref, DEGREE)
    node = zero
    for k in range(DEGREE):
        node = jnp.where(row == k, row_of(ct_ref, k), node)
    node = mul2((node, zero), (scale, zero))

    def applied(c):
        return cadd(
            each(lambda v: pltpu.roll(v, 1, 0), c), (mul2(c[0], node), mul2(c[1], node))
        )

    def dot(a, b):
        return over_rows(cmul(conj(a), b))

    def with_first(c):
        return over_rows(cmul(first_row, c))

    def through_gram(c, count):
        out = None
        for j in range(count):
            term = cmul(columns[j], each(lambda v: jnp.broadcast_to(v[j : j + 1, :], (TILE, LANES)), c))
            out = term if out is None else cadd(out, term)
        return out

    one = jnp.where(row == 0, 1.0, 0.0).astype(F32)
    unit = ((one, zero), (zero, zero))
    nothing = ((zero, zero), (zero, zero))
    solution, residual, direction = nothing, unit, unit
    rho = with_first(unit)
    for iteration in range(ITERS):
        image = applied(direction)
        alpha = cdiv(rho, with_first(image))
        middle = cadd(residual, cneg(cmul(alpha, image)))
        second = applied(middle)
        weighted = through_gram(second, 2 * iteration + 3)
        size = dot(second, weighted)
        size = (size[0], (zero, zero))
        along = conj(dot(middle, weighted))
        weight = (div2(along[0], size[0]), div2(along[1], size[0]))
        solution = cadd(solution, cadd(cmul(alpha, direction), cmul(weight, middle)))
        residual = cadd(middle, cneg(cmul(weight, second)))
        if iteration + 1 < ITERS:
            following = cneg(cmul(weight, with_first(second)))
            beta = cmul(cdiv(following, rho), cdiv(alpha, weight))
            direction = cadd(
                residual, cmul(beta, cadd(direction, cneg(cmul(weight, image))))
            )
            rho = following
    solution = tuple(mul2(v, (scale, zero)) for v in solution)
    return solution, residual


def last_step_kernel(*refs):
    gathered, ct_ref, src = refs[:3]
    os, ns, xs = refs[3:9], refs[9:15], refs[15:21]
    x_hbm, r_hbm, x_ref, r_ref, sems = refs[21:]
    core = lax.axis_index("gy")
    half = src.shape[4]
    solution, residual = coefficients(gathered[:, 0, :], ct_ref)

    def spread(value):
        return [
            tuple(jnp.broadcast_to(part[0][j : j + 1, :], (TILE, LANES)) for part in value)
            for j in range(DEGREE + 1)
        ]

    cs, cr = spread(solution), spread(residual)
    own = half * core
    copies = []
    for c in range(3):
        for plane, refs_of, which, shift in (
            (3 * core, os, None, own),
            (1 + core, ns, None, own),
            (3 * (1 - core), xs, 0, 0),
            (2 - core, xs, 1, 0),
        ):
            for t in range(half // TILE):
                s = slice(t * TILE, (t + 1) * TILE)
                for h in range(2):
                    z = slice(h * LANES, (h + 1) * LANES)
                    vr, vi = src[0, c, 0, plane, s, z], src[0, c, 1, plane, s, z]
                    sol = times((vr, vi), cs[0])
                    res = times((vr, vi), cr[0])
                    for k in range(1, DEGREE + 1):
                        ref = refs_of[k - 1]
                        if which is None:
                            at = pl.ds(pl.multiple_of(shift + t * TILE, TILE), TILE)
                            v = ref[c, 0, h, at, :], ref[c, 1, h, at, :]
                        else:
                            v = ref[which, c, 0, h, s, :], ref[which, c, 1, h, s, :]
                        res = plus(res, times(v, cr[k]))
                        if k < DEGREE:
                            sol = plus(sol, times(v, cs[k]))
                    for part in range(2):
                        x_ref[c, part, plane, s, z] = sol[part]
                        r_ref[c, part, plane, s, z] = res[part]
        for n, (a, b) in enumerate(((x_ref, x_hbm), (r_ref, r_hbm))):
            copy = pltpu.make_async_copy(a.at[c], b.at[0, c], sems.at[n, c])
            copy.start()
            copies.append(copy)
    for copy in copies:
        copy.wait()


def body(source, permittivity, frequency):
    cells_x, rows, depth = source.shape[3:]
    chips = lax.axis_size("gx")
    core = lax.axis_index("gy")
    both = [(0, 1), (1, 0)]
    ring = [(2 * i + 1, (2 * i + 2) % (2 * chips)) for i in range(chips)]
    ring = ring + [(b, a) for a, b in ring]

    def shape(*dims):
        return jax.ShapeDtypeStruct(dims, F32)

    def cost(flops):
        return pl.CostEstimate(flops=flops, bytes_accessed=0, transcendentals=0)

    half_x = cells_x // 2
    away = half_x * (1 - core)
    src_in = lax.ppermute(
        lax.dynamic_slice_in_dim(source[0], away, half_x, axis=2), "gy", both
    )
    eps_in = lax.ppermute(
        lax.dynamic_slice_in_dim(permittivity, away, half_x, axis=1), "gy", both
    )
    ny = 2 * rows
    field, pair = shape(3, 2, 2, ny, LANES), shape(2, 2, 2, ny, LANES)
    medium = shape(3, 2, ny, LANES)
    o, n, mo, mn, go, gn, off, on, cy, cz, cx, ct = pl.pallas_call(
        functools.partial(start_kernel, cells_x),
        out_shape=[
            field, field, medium, medium, pair, pair, pair, pair,
            shape(4, ny, LANES), shape(TILE, LANES), shape(2 * TILE, LANES), shape(TILE, LANES),
        ],
        in_specs=[VMEM] * 5,
        out_specs=[VMEM] * 12,
        compiler_params=params(12),
        name="start",
    )(source, permittivity, src_in, eps_in, frequency.reshape(1, 1))

    def plane(outer, k, p, q, gq, halo, m):
        return pl.pallas_call(
            functools.partial(plane_kernel, outer, k),
            out_shape=[field, pair, pair],
            in_specs=[VMEM] * 9,
            out_specs=[VMEM] * 3,
            compiler_params=params(12),
            cost_estimate=cost(2_000_000),
            name=("outer" if outer else "inner") + str(k),
        )(p, q, gq, halo, m, cy, cz, cx, ct)

    def gram(k, copies, os, ns, row):
        outs = [shape(1, LANES) if copies == 1 else shape(copies, 1, LANES)]
        if k:
            outs.append(shape(2, 3, 2, 2, rows, LANES))
        args = [*os[: k + 1], *ns[: k + 1]] + ([row] if k else [])
        got = pl.pallas_call(
            functools.partial(gram_kernel, k, copies),
            out_shape=outs,
            in_specs=[VMEM] * len(args),
            out_specs=[VMEM] * len(outs),
            compiler_params=params(12),
            cost_estimate=cost(500_000 * (k + 1)),
            name="gram" + str(k),
        )(*args)
        return (got[0], lax.ppermute(got[1], "gy", both)) if k else (got[0], None)

    os, ns, xs = [o], [n], []
    row = None
    for k in range(DEGREE):
        far = lax.ppermute(off, ("gx", "gy"), ring)
        near = lax.ppermute(on, "gy", both)
        row, x = gram(k, 1, os, ns, row)
        if k:
            xs.append(x)
        o2, go2, off = plane(True, k, os[k], ns[k], gn, far, mo)
        n2, gn2, on = plane(False, k, ns[k], os[k], go, near, mn)
        go, gn = go2, gn2
        os.append(o2)
        ns.append(n2)
    row, x = gram(DEGREE, 2 * chips, os, ns, row)
    xs.append(x)
    gathered = lax.all_to_all(row, ("gx", "gy"), split_axis=0, concat_axis=0, tiled=True)
    whole = shape(*source.shape)
    local = pltpu.VMEM(source.shape[1:], F32)
    return tuple(
        pl.pallas_call(
            last_step_kernel,
            out_shape=[whole, whole],
            in_specs=[VMEM] * 21,
            out_specs=[ANY, ANY],
            scratch_shapes=[local, local, pltpu.SemaphoreType.DMA((2, 3))],
            compiler_params=params(16),
            name="combine",
        )(gathered, ct, source, *os[1:], *ns[1:], *xs)
    )


def solution(mesh):
    placed = (P("groups", None, None, "gx", "gy", None), P("groups", "gx", "gy", None), P())
    out = P("groups", None, None, "gx", "gy", None)
    return jax.shard_map(body, mesh=mesh, in_specs=placed, out_specs=(out, out), check_vma=False)
```

```python
import functools

import jax
import jax.numpy as jnp
from jax import lax
from jax.experimental import pallas as pl
from jax.experimental.pallas import tpu as pltpu
from jax.sharding import PartitionSpec as P

PML = 8
ITERS = 3
DEGREE = 2 * ITERS
pml_strength = 2.0
LANES = 128
TILE = 8
COMBINE_MIB = 12

NODES = (0.0, -1.0, 1.0, 0.577, -0.671, 0.319)
F32 = jnp.float32
VMEM = pl.BlockSpec(memory_space=pltpu.VMEM)
ANY = pl.BlockSpec(memory_space=pl.ANY)
HBM = pl.BlockSpec(memory_space=pltpu.HBM)


def params(mib):
    return pltpu.CompilerParams(vmem_limit_bytes=int(mib * 2**20))


def stretch(points, length, frequency):
    inside = jnp.maximum(jnp.maximum(PML - points, points - (length - PML)), 0.0) / PML
    damping = pml_strength * inside * inside * inside / frequency
    factor = 1.0 / (1.0 + damping * damping)
    return factor, -damping * factor


def times(value, factor):
    return (
        value[0] * factor[0] - value[1] * factor[1],
        value[0] * factor[1] + value[1] * factor[0],
    )


def minus(a, b):
    return a[0] - b[0], a[1] - b[1]


def plus(a, b):
    return a[0] + b[0], a[1] + b[1]


def iota(shape, axis):
    return lax.broadcasted_iota(jnp.int32, shape, axis)


class Line:
    def __init__(self):
        self.lane = iota((TILE, LANES), 1)
        self.row = iota((TILE, LANES), 0)
        self.zero = jnp.zeros((TILE, LANES), F32)

    def z_next(self, low, high):
        low, high = pltpu.roll(low, LANES - 1, 1), pltpu.roll(high, LANES - 1, 1)
        last = self.lane == LANES - 1
        return jnp.where(last, high, low), jnp.where(last, 0.0, high)

    def z_before(self, low, high):
        low, high = pltpu.roll(low, 1, 1), pltpu.roll(high, 1, 1)
        first = self.lane == 0
        return jnp.where(first, 0.0, low), jnp.where(first, low, high)

    def up(self, tile):
        return pltpu.roll(tile, TILE - 1, 0)

    def down(self, tile):
        return pltpu.roll(tile, 1, 0)

    def y_next(self, rolled, rolled_after):
        return jnp.where(self.row == TILE - 1, rolled_after, rolled)

    def y_before(self, rolled, rolled_ahead):
        return jnp.where(self.row == 0, rolled_ahead, rolled)


def z_steps(line, pair):
    out = []
    for part in range(2):
        low, high = pair[0][part], pair[1][part]
        a, b = line.z_next(low, high)
        out.append((a - low, b - high))
    return [(out[0][h], out[1][h]) for h in range(2)]


def z_steps_back(line, pair):
    out = []
    for part in range(2):
        low, high = pair[0][part], pair[1][part]
        a, b = line.z_before(low, high)
        out.append((low - a, high - b))
    return [(out[0][h], out[1][h]) for h in range(2)]


def row_of(ref, at):
    return jnp.broadcast_to(ref[at : at + 1, :], (TILE, LANES))


def complex_row(ref, at):
    return row_of(ref, at), row_of(ref, at + 1)


def is_stretched(t, tiles):
    return t * TILE < PML or (t + 1) * TILE > tiles * TILE - PML


def edge_terms(line, field, t, tiles, fz, fx, y_front, store):
    now = field(t)
    after = field(t + 1) if t + 1 < tiles else None
    dz = z_steps(line, now[0])
    for h in range(2):
        gy = plus(times(dz[h], fz[h]), times(now[2][h], fx))
        dy = []
        for part in range(2):
            rolled = line.up(now[0][h][part])
            nxt = line.up(after[0][h][part]) if after is not None else line.zero
            dy.append(line.y_next(rolled, nxt) - now[0][h][part])
        if is_stretched(t, tiles):
            dy = times(dy, y_front(t))
        gz = minus((-dy[0], -dy[1]), times(now[1][h], fx))
        for part in range(2):
            store(0, part, h, t, gy[part])
            store(1, part, h, t, gz[part])


def tile_reader(ref, components=3):
    def read(t):
        s = slice(t * TILE, (t + 1) * TILE)
        return [
            [(ref[c, 0, h, s, :], ref[c, 1, h, s, :]) for h in range(2)] for c in range(components)
        ]

    return read


def tile_writer(ref):
    def write(c, part, h, t, value):
        ref[c, part, h, t * TILE : (t + 1) * TILE, :] = value

    return write


def split_kernel(count, s_hbm, e_hbm, *refs):
    core = lax.axis_index("gy")
    sems = refs[4]
    copies = []
    for n, whose in enumerate((1 - core, core)):
        at = pl.ds(count * whose, count)
        copies.append(pltpu.make_async_copy(s_hbm.at[0, :, :, at], refs[2 * n], sems.at[2 * n]))
        copies.append(pltpu.make_async_copy(e_hbm.at[:, at], refs[2 * n + 1], sems.at[2 * n + 1]))
    for copy in copies:
        copy.start()
    for copy in copies:
        copy.wait()


def start_kernel(
    cells_x, src, eps, src_in, eps_in, freq,
    o_ref, n_ref, mo_ref, mn_ref, go_ref, gn_ref, off_ref, on_ref, cy_ref, cz_ref, cx_ref, ct_ref,
):
    core = lax.axis_index("gy")
    chip = lax.axis_index("gx")
    rows, cols = src.shape[3], src.shape[4]
    ny, nx = 2 * rows, cells_x * lax.axis_size("gx")
    half_x = cells_x // 2
    tiles = ny // TILE
    f = jnp.broadcast_to(freq[...], (TILE, LANES))
    square = f * f

    def arrange(first_own):
        own_rows = slice(rows * first_own, rows * (first_own + 1))
        other_rows = slice(rows * (1 - first_own), rows * (2 - first_own))
        for dest, mdest, plane in ((o_ref, mo_ref, first_own), (n_ref, mn_ref, 1 - first_own)):
            for h in range(2):
                z = slice(h * LANES, (h + 1) * LANES)
                for c in range(3):
                    for part in range(2):
                        dest[c, part, h, own_rows, :] = src[c, part, plane, :, z]
                        dest[c, part, h, other_rows, :] = src_in[c, part, plane, :, z]
                    scale = square[0:1, :]
                    mdest[c, h, own_rows, :] = eps[c, plane, :, z] * scale
                    mdest[c, h, other_rows, :] = eps_in[c, plane, :, z] * scale

    @pl.when(core == 0)
    def _():
        arrange(0)

    @pl.when(core != 0)
    def _():
        arrange(1)

    fy = jnp.broadcast_to(freq[...], (ny, LANES))
    y = iota((ny, LANES), 0).astype(F32)
    cy_ref[0], cy_ref[1] = stretch(y + 0.5, ny, fy)
    cy_ref[2], cy_ref[3] = stretch(y, ny, fy)
    lane = iota((TILE, LANES), 1)
    for h in range(2):
        z = (lane + h * LANES).astype(F32)
        for i, value in enumerate((*stretch(z + 0.5, cols, f), *stretch(z, cols, f))):
            cz_ref[4 * h + i : 4 * h + i + 1, :] = value[0:1, :]
    base = chip * cells_x + core * half_x
    for at, plane in ((0, core), (TILE, 1 - core)):
        x = (jnp.zeros((TILE, LANES), jnp.int32) + (base + plane)).astype(F32)
        values = (*stretch(x - 0.5, nx, f), *stretch(x + 0.5, nx, f), *stretch(x, nx, f))
        for i, value in enumerate(values):
            cx_ref[at + i : at + i + 1, :] = value[0:1, :]
    low = square * -12.0
    centre, radius = (12.0 + low) * 0.5, (12.0 - low) * 0.5
    for k, node in enumerate(NODES):
        ct_ref[k : k + 1, :] = (centre + radius * node)[0:1, :]
    ct_ref[DEGREE : DEGREE + 1, :] = (2.0 / radius)[0:1, :]

    line = Line()
    fz = [complex_row(cz_ref, 4 * h) for h in range(2)]

    def y_front(t):
        s = slice(t * TILE, (t + 1) * TILE)
        return cy_ref[0, s, :], cy_ref[1, s, :]

    for ref, g_ref, at in ((o_ref, go_ref, 0), (n_ref, gn_ref, TILE)):
        for t in range(tiles):
            edge_terms(
                line, tile_reader(ref), t, tiles, fz, complex_row(cx_ref, at + 2), y_front,
                tile_writer(g_ref),
            )

    @pl.when(core == 0)
    def _():
        off_ref[...] = o_ref[1:3]
        on_ref[...] = gn_ref[...]

    @pl.when(core != 0)
    def _():
        off_ref[...] = go_ref[...]
        on_ref[...] = n_ref[1:3]


def plane_kernel(outer, k, *refs):
    refs = list(refs)
    p_ref, q_ref, gq_ref, halo_ref, m_ref, cy_ref, cz_ref, cx_ref, ct_ref = refs[:9]
    refs = refs[9:]
    last = k + 1 == DEGREE
    new_ref = refs[0]
    g_ref, out_ref = (None, None) if last else refs[1:]
    give_ref = refs[1] if last else None
    core = lax.axis_index("gy")
    chip = lax.axis_index("gx")
    tiles = p_ref.shape[3] // TILE
    at = 0 if outer else TILE
    line = Line()
    before = complex_row(cx_ref, at)
    fx = complex_row(cx_ref, at + 2)
    bx = complex_row(cx_ref, at + 4)
    fz = [complex_row(cz_ref, 4 * h) for h in range(2)]
    bz = [complex_row(cz_ref, 4 * h + 2) for h in range(2)]
    node = row_of(ct_ref, k)
    scale = row_of(ct_ref, DEGREE)

    def y_factor(first, t):
        s = slice(t * TILE, (t + 1) * TILE)
        return cy_ref[first, s, :], cy_ref[first + 1, s, :]

    def run(left):
        zero = line.zero
        edge = left and outer
        wall = outer and not left
        at_edge = (chip == 0) if edge else (chip == lax.axis_size("gx") - 1)
        closed = jnp.zeros((TILE, LANES), jnp.int32) + at_edge.astype(jnp.int32) > 0
        read_p = tile_reader(p_ref)
        halo_reader = tile_reader(halo_ref, 2)
        read_g = halo_reader if left else tile_reader(gq_ref, 2)
        if left:
            read_r = lambda t: tile_reader(q_ref)(t)[1:]
        else:
            read_r = halo_reader
        rolled_h = None
        pending = None
        nxt = read_p(0)
        rolled = [[[line.up(nxt[c][h][i]) for i in range(2)] for h in range(2)] for c in (0, 2)]
        write_new = tile_writer(new_ref)
        if not last:
            write_g = tile_writer(g_ref)
            write_out = tile_writer(out_ref)
            write_edge = write_g if left else write_out

        def finish(pend, after):
            t0, ex, rolled_ex, base = pend
            for h in range(2):
                dy = [
                    line.y_next(rolled_ex[h][i], after[h][i] if after is not None else zero) - ex[h][i]
                    for i in range(2)
                ]
                if is_stretched(t0, tiles):
                    dy = times(dy, y_factor(0, t0))
                for i in range(2):
                    write_edge(1, i, h, t0, base[h][i] - dy[i])

        for t in range(tiles):
            ex, ey, ez = nxt
            if t + 1 < tiles:
                nxt = read_p(t + 1)
                rolled_next = [
                    [[line.up(nxt[c][h][i]) for i in range(2)] for h in range(2)] for c in (0, 2)
                ]
            else:
                rolled_next = [[[zero] * 2] * 2] * 2
            gl, right = read_g(t), read_r(t)
            pml = is_stretched(t, tiles)
            dz_y, dz_x = z_steps(line, ey), z_steps(line, ex)
            hx, hy, hz, cross_y, cross_z = [], [], [], [], []
            for h in range(2):
                dy_x, dy_z = (
                    [
                        line.y_next(rolled[j][h][i], rolled_next[j][h][i]) - field[h][i]
                        for i in range(2)
                    ]
                    for j, field in ((0, ex), (1, ez))
                )
                if pml:
                    dy_x, dy_z = times(dy_x, y_factor(0, t)), times(dy_z, y_factor(0, t))
                r_y, r_z = right[0][h], right[1][h]
                if wall:
                    r_y = [jnp.where(closed, 0.0, r) for r in r_y]
                    r_z = [jnp.where(closed, 0.0, r) for r in r_z]
                hx.append(minus(dy_z, times(dz_y[h], fz[h])))
                hy.append(minus(times(dz_x[h], fz[h]), times(minus(r_z, ez[h]), fx)))
                hz.append(minus(times(minus(r_y, ey[h]), fx), dy_x))
                l_y = minus(gl[0][h], times(ez[h], before))
                l_z = plus(gl[1][h], times(ey[h], before))
                if edge:
                    l_y = [jnp.where(closed, 0.0, v) for v in l_y]
                    l_z = [jnp.where(closed, 0.0, v) for v in l_z]
                cross_y.append(times(minus(hy[h], l_y), bx))
                cross_z.append(times(minus(hz[h], l_z), bx))
            rolled = rolled_next
            new_rolled = [[[line.down(v[h][i]) for i in range(2)] for h in range(2)] for v in (hx, hz)]
            bz_y, bz_x = z_steps_back(line, hy), z_steps_back(line, hx)
            s = slice(t * TILE, (t + 1) * TILE)
            made = [[], [], []]
            for h in range(2):
                by_x, by_z = (
                    [
                        field[h][i]
                        - line.y_before(
                            new_rolled[j][h][i], rolled_h[j][h][i] if rolled_h is not None else zero
                        )
                        for i in range(2)
                    ]
                    for j, field in ((0, hx), (1, hz))
                )
                if pml:
                    by_x, by_z = times(by_x, y_factor(2, t)), times(by_z, y_factor(2, t))
                curls = (
                    minus(by_z, times(bz_y[h], bz[h])),
                    minus(times(bz_x[h], bz[h]), cross_z[h]),
                    minus(cross_y[h], by_x),
                )
                for c, (curl, field) in enumerate(zip(curls, (ex, ey, ez))):
                    shifted = m_ref[c, h, s, :] + node
                    made[c].append([(curl[i] - shifted * field[h][i]) * scale for i in range(2)])
                    for i in range(2):
                        write_new(c, i, h, t, made[c][h][i])
                        if left and c and not last:
                            write_out(c - 1, i, h, t, made[c][h][i])
            rolled_h = new_rolled
            if last:
                continue
            dz = z_steps(line, made[0])
            up = [[line.up(made[0][h][i]) for i in range(2)] for h in range(2)]
            base = []
            for h in range(2):
                gy = plus(times(dz[h], fz[h]), times(made[2][h], fx))
                for i in range(2):
                    write_edge(0, i, h, t, gy[i])
                b = times(made[1][h], fx)
                base.append((-b[0], -b[1]))
            if pending is not None:
                finish(pending, up)
            pending = (t, made[0], up, base)
        if not last:
            finish(pending, None)
        else:
            half = tiles * TILE // 2
            rows = slice(half, 2 * half) if left == outer else slice(0, half)
            give_ref[...] = new_ref[:, :, :, rows, :]

    left_here = (core == 0) if outer else (core != 0)

    @pl.when(left_here)
    def _():
        run(True)

    @pl.when(jnp.logical_not(left_here))
    def _():
        run(False)


def two_sum(a, b):
    s = a + b
    v = s - a
    return s, (a - (s - v)) + (b - v)


def total_of(tile):
    top = jnp.max(jnp.max(jnp.abs(tile), axis=1, keepdims=True), axis=0, keepdims=True)
    shift = top * 1024.0
    lead = (tile + shift) - shift
    rest = tile - lead
    add = lambda v: jnp.sum(jnp.sum(v, axis=1, keepdims=True), axis=0, keepdims=True)
    return add(lead), add(rest)


def gram_kernel(k, copies, *refs):
    count = k + 1
    os, ns = refs[:count], refs[count : 2 * count]
    rest = list(refs[2 * count :])
    row_in = rest.pop(0) if k else None
    store = 0 < k < DEGREE
    if store and k > 1:
        rest = rest[2:]
    row_ref = rest.pop(0)
    core = lax.axis_index("gy")
    rows = os[0].shape[3]
    half = rows // 2
    pending = []
    if store:
        own_ref, give_ref, sems = rest
        for to, (ref, whose) in enumerate(((own_ref, core), (give_ref, 1 - core))):
            part = pl.ds(pl.multiple_of(half * whose, TILE), half)
            for n, source in enumerate((os[k], ns[k])):
                pending.append(
                    pltpu.make_async_copy(
                        source.at[:, :, :, part], ref.at[k - 1, n], sems.at[to, n]
                    )
                )
    for copy in pending:
        copy.start()
    tiles = rows // TILE
    zero = jnp.zeros((TILE, LANES), F32)
    real = [[zero, zero] for _ in range(count)]
    imag = [[zero, zero] for _ in range(count)]
    for which, group in enumerate((os, ns)):
        for c in range(3):
            for h in range(2):
                for t in range(tiles):
                    s = slice(t * TILE, (t + 1) * TILE)
                    ar, ai = group[k][c, 0, h, s, :], group[k][c, 1, h, s, :]
                    for i in range(k):
                        br, bi = group[i][c, 0, h, s, :], group[i][c, 1, h, s, :]
                        real[i][which] += br * ar + bi * ai
                        imag[i][which] += br * ai - bi * ar
                    real[k][which] += ar * ar + ai * ai
    lane = iota((1, LANES), 1)
    row = row_in[...] if k else jnp.zeros((1, LANES), F32)
    for i in range(count):
        lead, less = total_of(real[i][0] + real[i][1])
        row = jnp.where(lane == 8 * i + k, lead, row)
        row = jnp.where(lane == 64 + 8 * i + k, less, row)
        if i < k:
            lead, less = total_of(imag[i][0] + imag[i][1])
            row = jnp.where(lane == 8 * k + i, lead, row)
            row = jnp.where(lane == 64 + 8 * k + i, less, row)
    if copies == 1:
        row_ref[...] = row
    else:
        for d in range(copies):
            row_ref[d] = row
    for copy in pending:
        copy.wait()


def quick(a, b):
    s = a + b
    return s, b - (s - a)


def add2(a, b):
    s, e = two_sum(a[0], b[0])
    return quick(s, e + (a[1] + b[1]))


def neg2(a):
    return -a[0], -a[1]


def split(a):
    c = a * 4097.0
    high = c - (c - a)
    return high, a - high


def mul2(a, b):
    p = a[0] * b[0]
    (a1, a2), (b1, b2) = split(a[0]), split(b[0])
    e = ((a1 * b1 - p) + a1 * b2 + a2 * b1) + a2 * b2
    return quick(p, e + (a[0] * b[1] + a[1] * b[0]))


def div2(a, b):
    q = a[0] / b[0]
    rest = add2(a, neg2(mul2((q, jnp.zeros_like(q)), b)))
    q2 = rest[0] / b[0]
    rest = add2(rest, neg2(mul2((q2, jnp.zeros_like(q)), b)))
    return add2(quick(q, q2), (rest[0] / b[0], jnp.zeros_like(q)))


def cadd(a, b):
    return add2(a[0], b[0]), add2(a[1], b[1])


def cneg(a):
    return neg2(a[0]), neg2(a[1])


def conj(a):
    return a[0], neg2(a[1])


def cmul(a, b):
    return (
        add2(mul2(a[0], b[0]), neg2(mul2(a[1], b[1]))),
        add2(mul2(a[0], b[1]), mul2(a[1], b[0])),
    )


def cdiv(a, b):
    size = add2(mul2(b[0], b[0]), mul2(b[1], b[1]))
    top = cmul(a, conj(b))
    return div2(top[0], size), div2(top[1], size)


def each(fn, a):
    return tuple((fn(p[0]), fn(p[1])) for p in a)


def over_rows(a):
    for d in (4, 2, 1):
        a = cadd(a, each(lambda v: pltpu.roll(v, d, 0), a))
    return a


def coefficients(gathered, ct_ref):
    parts = [gathered[i * TILE : (i + 1) * TILE] for i in range(gathered.shape[0] // TILE)]
    parts = [(p, jnp.zeros_like(p)) for p in parts]
    while len(parts) > 1:
        parts = [add2(parts[2 * i], parts[2 * i + 1]) for i in range(len(parts) // 2)]
    total = parts[0]
    for d in (4, 2, 1):
        total = add2(total, tuple(pltpu.roll(v, d, 0) for v in total))
    other = tuple(pltpu.roll(v, 64, 1) for v in total)
    total = add2(total, other)
    row, lane = iota((TILE, LANES), 0), iota((TILE, LANES), 1)

    def picked(mask):
        return tuple(
            jnp.broadcast_to(
                jnp.sum(jnp.where(mask, v, 0.0), axis=1, keepdims=True), (TILE, LANES)
            )
            for v in total
        )

    columns = []
    for j in range(DEGREE + 1):
        real = picked(lane == 8 * jnp.minimum(row, j) + jnp.maximum(row, j))
        imag = picked((lane == 8 * jnp.maximum(row, j) + jnp.minimum(row, j)) & (row != j))
        imag = tuple(jnp.where(row > j, -v, v) for v in imag)
        columns.append((real, imag))
    zero = jnp.zeros((TILE, LANES), F32)
    first_row = conj(columns[0])
    scale = row_of(ct_ref, DEGREE)
    node = zero
    for k in range(DEGREE):
        node = jnp.where(row == k, row_of(ct_ref, k), node)
    node = mul2((node, zero), (scale, zero))

    def applied(c):
        return cadd(
            each(lambda v: pltpu.roll(v, 1, 0), c), (mul2(c[0], node), mul2(c[1], node))
        )

    def dot(a, b):
        return over_rows(cmul(conj(a), b))

    def with_first(c):
        return over_rows(cmul(first_row, c))

    def through_gram(c, count):
        out = None
        for j in range(count):
            term = cmul(columns[j], each(lambda v: jnp.broadcast_to(v[j : j + 1, :], (TILE, LANES)), c))
            out = term if out is None else cadd(out, term)
        return out

    one = jnp.where(row == 0, 1.0, 0.0).astype(F32)
    unit = ((one, zero), (zero, zero))
    nothing = ((zero, zero), (zero, zero))
    solution, residual, direction = nothing, unit, unit
    rho = with_first(unit)
    for iteration in range(ITERS):
        image = applied(direction)
        alpha = cdiv(rho, with_first(image))
        middle = cadd(residual, cneg(cmul(alpha, image)))
        second = applied(middle)
        weighted = through_gram(second, 2 * iteration + 3)
        size = dot(second, weighted)
        size = (size[0], (zero, zero))
        along = conj(dot(middle, weighted))
        weight = (div2(along[0], size[0]), div2(along[1], size[0]))
        solution = cadd(solution, cadd(cmul(alpha, direction), cmul(weight, middle)))
        residual = cadd(middle, cneg(cmul(weight, second)))
        if iteration + 1 < ITERS:
            following = cneg(cmul(weight, with_first(second)))
            beta = cmul(cdiv(following, rho), cdiv(alpha, weight))
            direction = cadd(
                residual, cmul(beta, cadd(direction, cneg(cmul(weight, image))))
            )
            rho = following
    solution = tuple(mul2(v, (scale, zero)) for v in solution)
    return solution, residual


def last_step_kernel(*refs):
    gathered, ct_ref, src, own_ref, got_ref, o_last, n_last, o_got, n_got = refs[:9]
    x_hbm, r_hbm, v0_ref, v_ref, x_ref, r_ref, first_sems, in_sems, sems = refs[9:]
    core = lax.axis_index("gy")
    half = v_ref.shape[5]
    coming = [[] for _ in range(3)]
    for c in range(3):
        coming[c].append(pltpu.make_async_copy(src.at[0, c], v0_ref.at[c], first_sems.at[c]))
        for n, (ref, plane) in enumerate(
            (
                (own_ref.at[:, 0], 3 * core),
                (own_ref.at[:, 1], 1 + core),
                (got_ref.at[:, 0], 3 * (1 - core)),
                (got_ref.at[:, 1], 2 - core),
            )
        ):
            coming[c].append(
                pltpu.make_async_copy(
                    ref.at[:, c], v_ref.at[: DEGREE - 1, c, :, :, plane], in_sems.at[c, n]
                )
            )
        mine = pl.ds(pl.multiple_of(half * core, TILE), half)
        for n, (ref, plane) in enumerate(
            (
                (o_last.at[c, :, :, mine], 3 * core),
                (n_last.at[c, :, :, mine], 1 + core),
                (o_got.at[c], 3 * (1 - core)),
                (n_got.at[c], 2 - core),
            )
        ):
            coming[c].append(
                pltpu.make_async_copy(
                    ref, v_ref.at[DEGREE - 1, c, :, :, plane], in_sems.at[c, 4 + n]
                )
            )
    for copies in coming:
        for copy in copies:
            copy.start()
    solution, residual = coefficients(gathered[:, 0, :], ct_ref)

    def spread(value):
        return [
            tuple(jnp.broadcast_to(part[0][j : j + 1, :], (TILE, LANES)) for part in value)
            for j in range(DEGREE + 1)
        ]

    cs, cr = spread(solution), spread(residual)
    leaving = []
    for c in range(3):
        for copy in coming[c]:
            copy.wait()
        for plane in range(v_ref.shape[4]):
            for t in range(half // TILE):
                s = slice(t * TILE, (t + 1) * TILE)
                for h in range(2):
                    z = slice(h * LANES, (h + 1) * LANES)
                    v = v0_ref[c, 0, plane, s, z], v0_ref[c, 1, plane, s, z]
                    sol = times(v, cs[0])
                    res = times(v, cr[0])
                    for k in range(1, DEGREE + 1):
                        v = v_ref[k - 1, c, 0, h, plane, s, :], v_ref[k - 1, c, 1, h, plane, s, :]
                        res = plus(res, times(v, cr[k]))
                        if k < DEGREE:
                            sol = plus(sol, times(v, cs[k]))
                    for part in range(2):
                        x_ref[c, part, plane, s, z] = sol[part]
                        r_ref[c, part, plane, s, z] = res[part]
        for n, (a, b) in enumerate(((x_ref, x_hbm), (r_ref, r_hbm))):
            copy = pltpu.make_async_copy(a.at[c], b.at[0, c], sems.at[n, c])
            copy.start()
            leaving.append(copy)
    for copy in leaving:
        copy.wait()


def body(source, permittivity, frequency):
    cells_x, rows, depth = source.shape[3:]
    chips = lax.axis_size("gx")
    core = lax.axis_index("gy")
    both = [(0, 1), (1, 0)]
    ring = [(2 * i + 1, (2 * i + 2) % (2 * chips)) for i in range(chips)]
    ring = ring + [(b, a) for a, b in ring]

    def shape(*dims):
        return jax.ShapeDtypeStruct(dims, F32)

    def cost(flops):
        return pl.CostEstimate(flops=flops, bytes_accessed=0, transcendentals=0)

    half_x = cells_x // 2
    share, share_eps = (3, 2, half_x, rows, depth), (3, half_x, rows, depth)
    moved, moved_eps, stays, stays_eps = pl.pallas_call(
        functools.partial(split_kernel, half_x),
        out_shape=[pltpu.VMEM(s, F32) for s in (share, share_eps) * 2],
        in_specs=[HBM] * 2,
        out_specs=[VMEM] * 4,
        scratch_shapes=[pltpu.SemaphoreType.DMA((4,))],
        compiler_params=params(62.5),
        name="split",
    )(source, permittivity)
    src_in = lax.ppermute(moved, "gy", both)
    eps_in = lax.ppermute(moved_eps, "gy", both)
    ny = 2 * rows
    field, pair = shape(3, 2, 2, ny, LANES), shape(2, 2, 2, ny, LANES)
    medium = shape(3, 2, ny, LANES)
    o, n, mo, mn, go, gn, off, on, cy, cz, cx, ct = pl.pallas_call(
        functools.partial(start_kernel, cells_x),
        out_shape=[
            field, field, medium, medium, pair, pair, pair, pair,
            shape(4, ny, LANES), shape(TILE, LANES), shape(2 * TILE, LANES), shape(TILE, LANES),
        ],
        in_specs=[VMEM] * 5,
        out_specs=[VMEM] * 12,
        compiler_params=params(4),
        name="start",
    )(stays, stays_eps, src_in, eps_in, frequency.reshape(1, 1))

    def plane(outer, k, p, q, gq, halo, m):
        outs = [field, shape(3, 2, 2, rows, LANES)] if k + 1 == DEGREE else [field, pair, pair]
        return pl.pallas_call(
            functools.partial(plane_kernel, outer, k),
            out_shape=outs,
            in_specs=[VMEM] * 9,
            out_specs=[VMEM] * len(outs),
            compiler_params=params(2),
            cost_estimate=cost(2_000_000),
            name=("outer" if outer else "inner") + str(k),
        )(p, q, gq, halo, m, cy, cz, cx, ct)

    halves = pltpu.HBM((DEGREE - 1, 2, 3, 2, 2, rows, LANES), F32)

    def gram(k, copies, os, ns, row, held):
        store = 0 < k < DEGREE
        outs = [shape(1, LANES) if copies == 1 else shape(copies, 1, LANES)]
        args = [*os[: k + 1], *ns[: k + 1]] + ([row] if k else [])
        specs = [VMEM] * len(args)
        aliases = {}
        if store and k > 1:
            aliases = {len(args): 1, len(args) + 1: 2}
            args += held
            specs += [HBM] * 2
        return pl.pallas_call(
            functools.partial(gram_kernel, k, copies),
            out_shape=outs + ([halves] * 2 if store else []),
            in_specs=specs,
            out_specs=[VMEM] + ([HBM] * 2 if store else []),
            input_output_aliases=aliases,
            scratch_shapes=[pltpu.SemaphoreType.DMA((2, 2))] if store else [],
            compiler_params=params(2),
            cost_estimate=cost(500_000 * (k + 1)),
            name="gram" + str(k),
        )(*args)

    os, ns, held = [o], [n], []
    row = None
    far = lax.ppermute(off, ("gx", "gy"), ring)
    for k in range(DEGREE):
        last = k + 1 == DEGREE
        row, *held = gram(k, 1, os, ns, row, held)
        if k:
            on, row = lax.optimization_barrier((on, row))
        near = lax.ppermute(on, "gy", both)
        o2, *edges = plane(True, k, os[k], ns[k], gn, far, mo)
        if last:
            own, give = held
            lasts = edges
            lasts[0], give, near = lax.optimization_barrier((lasts[0], give, near))
            got = lax.ppermute(give, "gy", both)
        else:
            go2, off = edges
            far = lax.ppermute(off, ("gx", "gy"), ring)
        n2, *edges = plane(False, k, ns[k], os[k], go, near, mn)
        if last:
            lasts += edges
        else:
            gn, on = edges
            go = go2
        os.append(o2)
        ns.append(n2)
    lasts = [lax.ppermute(a, "gy", both) for a in lasts]
    row = gram(DEGREE, 2 * chips, os, ns, row, None)[0]
    gathered = lax.all_to_all(row, ("gx", "gy"), split_axis=0, concat_axis=0, tiled=True)
    whole = shape(*source.shape)
    local = pltpu.VMEM(source.shape[1:], F32)
    return tuple(
        pl.pallas_call(
            last_step_kernel,
            out_shape=[whole, whole],
            in_specs=[VMEM] * 2 + [HBM] * 3 + [ANY] * 4,
            out_specs=[HBM, HBM],
            scratch_shapes=[
                local,
                pltpu.VMEM((DEGREE, 3, 2, 2, cells_x, rows, LANES), F32),
                local,
                local,
                pltpu.SemaphoreType.DMA((3,)),
                pltpu.SemaphoreType.DMA((3, 8)),
                pltpu.SemaphoreType.DMA((2, 3)),
            ],
            compiler_params=params(COMBINE_MIB),
            name="combine",
        )(gathered, ct, source, own, got, os[-1], ns[-1], *lasts)
    )


def solution(mesh):
    placed = (P("groups", None, None, "gx", "gy", None), P("groups", "gx", "gy", None), P())
    out = P("groups", None, None, "gx", "gy", None)
    return jax.shard_map(body, mesh=mesh, in_specs=placed, out_specs=(out, out), check_vma=False)
```
